32 devices in a mesh: wide: 8 (over z, x), group: 4 (over y, core).
Axes of the slice: x: 2, y: 2, z: 4, core: 2. Of those that a mesh axis runs over, the one named last changes fastest.
Arguments:
- feat4: bfloat16 [32, 24, 24, 256], P(('wide', 'group')), may hold values from -100 to 100
- feat5: bfloat16 [32, 12, 12, 256], P(('wide', 'group')), may hold values from -100 to 100
- feat6: bfloat16 [32, 6, 6, 256], P(('wide', 'group')), may hold values from -100 to 100
- feat7: bfloat16 [32, 3, 3, 256], P(('wide', 'group')), may hold values from -100 to 100
- out_grad4: bfloat16 [32, 24, 24, 256], P(('wide', 'group')), may hold values from -6 to 6
- out_grad5: bfloat16 [32, 12, 12, 256], P(('wide', 'group')), may hold values from -6 to 6
- out_grad6: bfloat16 [32, 6, 6, 256], P(('wide', 'group')), may hold values from -6 to 6
- out_grad7: bfloat16 [32, 3, 3, 256], P(('wide', 'group')), may hold values from -6 to 6
- conv_weight: bfloat16 [3, 3, 256, 256], replicated, may hold values from -0.125 to 0.125
- bn_gain: float32 [4, 256], replicated, may hold values from 0.25 to 1.75
- bn_shift: float32 [4, 256], replicated, may hold values from -0.5 to 0.5
- heights: int32 [32], P(('wide', 'group')), may hold values from 168 to 384
- widths: int32 [32], P(('wide', 'group')), may hold values from 168 to 384
Outputs:
- out4: bfloat16 [32, 24, 24, 256], P(('wide', 'group'))
- out5: bfloat16 [32, 12, 12, 256], P(('wide', 'group'))
- out6: bfloat16 [32, 6, 6, 256], P(('wide', 'group'))
- out7: bfloat16 [32, 3, 3, 256], P(('wide', 'group'))
- d_feat4: bfloat16 [32, 24, 24, 256], P(('wide', 'group'))
- d_feat5: bfloat16 [32, 12, 12, 256], P(('wide', 'group'))
- d_feat6: bfloat16 [32, 6, 6, 256], P(('wide', 'group'))
- d_feat7: bfloat16 [32, 3, 3, 256], P(('wide', 'group'))
- d_weight: float32 [3, 3, 256, 256], replicated
- d_gain: float32 [4, 256], replicated
- d_shift: float32 [4, 256], replicated
The draws below stay inside these ranges and needn't reach their ends.
Inputs may be any that keep to these rules, and one draw needn't show every extreme that they name: `heights`: pixel height of the valid part of each image. `widths`: pixel width of the valid part of each image.
All inputs are finite; a program needn't handle non-finite values.
Results may differ from the reference program's by a relative error of at most 0.0049.
Values sent between devices are 32-bit elements; how exact they have to be, the bound alone decides.
A program may use at most 64 MiB of HBM per device.

```python
from functools import partial
import jax
import jax.numpy as jnp
from jax import lax

CH = 256
SIDE4 = 24
LEVELS = 4
SIDE5 = 12
SIDE6 = 6
SIDE7 = 3
IMAGES = 32


def feature_values(key, extent):
    noise_key, offset_key = jax.random.split(key, 2)
    places = jnp.arange(IMAGES, dtype=jnp.float32) / max(IMAGES - 1, 1)
    image_ramp = 1.0 + 2.0 * places
    noise_part = jnp.clip(jax.random.normal(noise_key, (IMAGES, extent, extent, CH), jnp.float32), -6.0, 6.0)
    offset = jax.random.uniform(offset_key, (IMAGES, 1, 1, CH), jnp.float32, -0.5, 1.0)
    values = image_ramp[:, None, None, None] * (noise_part + offset)
    return values.astype(jnp.bfloat16)


def draw_feat4(key, part):
    return feature_values(jax.random.fold_in(key, 4), SIDE4)


def draw_feat5(key, part):
    return feature_values(jax.random.fold_in(key, 5), SIDE5)


def draw_feat6(key, part):
    return feature_values(jax.random.fold_in(key, 6), SIDE6)


def draw_feat7(key, part):
    return feature_values(jax.random.fold_in(key, 7), SIDE7)


def place_ends(entries, own_key, smallest, top_value):
    longest = entries.shape.index(max(entries.shape))
    spots = []
    for shift in (0, 1):
        where = [jax.random.randint(jax.random.fold_in(own_key, axis), (), 0, length) for axis, length in enumerate(entries.shape)]
        where[longest] = (where[longest] + shift) % entries.shape[longest]
        spots.append(tuple(where))
    return entries.at[spots[0]].set(smallest).at[spots[1]].set(top_value)


def block_levels(stream_key, shape, shards, smallest, largest):
    level = 1.0
    for position, parts in shards:
        draws = jax.random.uniform(jax.random.fold_in(jax.random.fold_in(stream_key, 6), position), (parts,), jnp.float32, smallest / len(shards), largest / len(shards))
        level = level * jnp.repeat(jnp.exp(draws), shape[position] // parts).reshape((-1,) + (1,) * (len(shape) - 1 - position))
    return level


def bell_draw(key, dims, spread, bound, cuts=(), held_as=jnp.bfloat16):
    entries = jax.random.normal(key, dims, jnp.float32) * spread
    if len(cuts) > 0:
        entries = block_levels(key, dims, cuts, -0.22, 0.18) * entries
    return jnp.clip(entries, min=-bound, max=bound).astype(held_as)


def setup_inputs(seed: int = 0) -> dict:
    streams_of = jax.random.split(jax.random.key(seed), 14)
    feat4 = draw_feat4(jax.random.fold_in(streams_of[13], 71), 0)
    feat5 = draw_feat5(jax.random.fold_in(streams_of[13], 71), 0)
    feat6 = draw_feat6(jax.random.fold_in(streams_of[13], 71), 0)
    feat7 = draw_feat7(jax.random.fold_in(streams_of[13], 71), 0)
    out_grad4 = bell_draw(streams_of[4], (IMAGES, SIDE4, SIDE4, CH), 1.0, 6.0, ((0, 32),))
    out_grad5 = bell_draw(streams_of[5], (IMAGES, SIDE5, SIDE5, CH), 1.0, 6.0, ((0, 32),))
    out_grad6 = bell_draw(streams_of[6], (IMAGES, SIDE6, SIDE6, CH), 1.0, 6.0, ((0, 32),))
    out_grad7 = bell_draw(streams_of[7], (IMAGES, SIDE7, SIDE7, CH), 1.0, 6.0, ((0, 32),))
    conv_weight = bell_draw(streams_of[8], (3, 3, CH, CH), (9 * CH) ** -0.5, 0.125)
    bn_gain = jnp.clip(1.0 + 0.15 * jax.random.normal(streams_of[9], (LEVELS, CH), jnp.float32), 0.25, 1.75)
    bn_shift = jnp.clip(jax.random.uniform(streams_of[10], (LEVELS, CH), jnp.float32, -0.5, 0.5), -0.5, 0.5)
    heights = place_ends(jax.random.randint(streams_of[11], (IMAGES,), SIDE4 * 7, SIDE4 * 16 + 1), jax.random.fold_in(streams_of[11], 1), SIDE4 * 7, SIDE4 * 16).astype(jnp.int32)
    widths = place_ends(jax.random.randint(streams_of[12], (IMAGES,), SIDE4 * 7, SIDE4 * 16 + 1), jax.random.fold_in(streams_of[12], 1), SIDE4 * 7, SIDE4 * 16).astype(jnp.int32)
    return {"feat4": feat4, "feat5": feat5, "feat6": feat6, "feat7": feat7, "out_grad4": out_grad4, "out_grad5": out_grad5, "out_grad6": out_grad6, "out_grad7": out_grad7, "conv_weight": conv_weight, "bn_gain": bn_gain, "bn_shift": bn_shift, "heights": heights, "widths": widths}


EPSILON = 1e-05

def level_masks(heights, widths, stride, extent):
    row_limit = (heights + stride - 1) // stride
    col_limit = (widths + stride - 1) // stride
    places = jnp.arange(extent, dtype=jnp.int32)
    inside = jnp.logical_and(places[None, :, None] < row_limit[:, None, None], places[None, None, :] < col_limit[:, None, None])
    return inside.astype(jnp.float32)

def conv_image(padded, conv_weight, extent):
    summed = jnp.zeros((extent * extent, conv_weight.shape[3]), jnp.float32)
    for tap_row in range(3):
        for tap_col in range(3):
            window = padded[tap_row:tap_row + extent, tap_col:tap_col + extent, :].reshape(extent * extent, -1)
            summed = summed + jnp.dot(window, conv_weight[tap_row, tap_col], preferred_element_type=jnp.float32)
    return summed.reshape(extent, extent, -1)

def input_grad_image(padded_back, conv_weight, extent):
    summed = jnp.zeros((extent * extent, conv_weight.shape[2]), jnp.float32)
    for tap_row in range(3):
        for tap_col in range(3):
            window = padded_back[2 - tap_row:2 - tap_row + extent, 2 - tap_col:2 - tap_col + extent, :].reshape(extent * extent, -1)
            summed = summed + lax.dot_general(window, conv_weight[tap_row, tap_col], (((1,), (1,)), ((), ())), preferred_element_type=jnp.float32)
    return summed.reshape(extent, extent, -1)

def weight_grad_image(padded, back_grad, extent):
    flat_back = back_grad.reshape(extent * extent, -1)
    tap_terms = []
    for tap_row in range(3):
        for tap_col in range(3):
            window = padded[tap_row:tap_row + extent, tap_col:tap_col + extent, :].reshape(extent * extent, -1)
            tap_terms.append(lax.dot_general(window, flat_back, (((0,), (0,)), ((), ())), preferred_element_type=jnp.float32))
    return jnp.stack(tap_terms).reshape(3, 3, padded.shape[2], flat_back.shape[1])

def reference(feat4, feat5, feat6, feat7, out_grad4, out_grad5, out_grad6, out_grad7, conv_weight, bn_gain, bn_shift, heights, widths):
    features = (feat4, feat5, feat6, feat7)
    cotangents = (out_grad4, out_grad5, out_grad6, out_grad7)
    outputs = []
    input_grads = []
    gain_rows = []
    shift_rows = []
    weight_total = jnp.zeros(conv_weight.shape, jnp.float32)
    for level_index in range(4):
        feature = features[level_index]
        extent = feature.shape[1]
        valid_mask = level_masks(heights, widths, 16 * 2 ** level_index, extent)
        weighted = valid_mask[..., None]
        masked = feature * weighted.astype(feature.dtype)
        padded = jnp.pad(masked, ((0, 0), (1, 1), (1, 1), (0, 0)))
        conv_out = lax.map(partial(conv_image, conv_weight=conv_weight, extent=extent), padded)
        pixel_count = jnp.sum(valid_mask)
        mean_value = lax.optimization_barrier(jnp.sum(conv_out * weighted, axis=(0, 1, 2))) / pixel_count
        centered = conv_out - mean_value
        variance = lax.optimization_barrier(jnp.sum(weighted * centered * centered, axis=(0, 1, 2))) / pixel_count
        inverse = lax.rsqrt(variance + EPSILON)
        normed = centered * inverse
        shifted = bn_gain[level_index] * normed + bn_shift[level_index]
        sigmoid_value = jax.nn.sigmoid(shifted)
        outputs.append((weighted * shifted * sigmoid_value).astype(jnp.bfloat16))
        slope_term = weighted * cotangents[level_index].astype(jnp.float32) * sigmoid_value * (1.0 + shifted * (1.0 - sigmoid_value))
        shift_sum = lax.optimization_barrier(jnp.sum(slope_term, axis=(0, 1, 2)))
        gain_sum = lax.optimization_barrier(jnp.sum(slope_term * normed, axis=(0, 1, 2)))
        back_grad = (weighted * (bn_gain[level_index] * inverse) * (slope_term - shift_sum / pixel_count - normed * (gain_sum / pixel_count))).astype(jnp.bfloat16)

        def add_image(carry_total, operands, extent=extent):
            return (carry_total + weight_grad_image(operands[0], operands[1], extent), None)
        weight_total, unused = lax.scan(add_image, weight_total, (padded, back_grad))
        padded_back = jnp.pad(back_grad, ((0, 0), (1, 1), (1, 1), (0, 0)))
        input_part = lax.map(partial(input_grad_image, conv_weight=conv_weight, extent=extent), padded_back)
        input_grads.append((weighted * input_part).astype(jnp.bfloat16))
        gain_rows.append(gain_sum)
        shift_rows.append(shift_sum)
    return (outputs[0], outputs[1], outputs[2], outputs[3], input_grads[0], input_grads[1], input_grads[2], input_grads[3], weight_total / IMAGES, jnp.stack(gain_rows) / IMAGES, jnp.stack(shift_rows) / IMAGES)
```

```python
import functools
import math

import jax
import jax.numpy as jnp
from jax import lax
from jax.experimental import pallas as pl
from jax.experimental.pallas import tpu as pltpu
from jax.sharding import PartitionSpec as P

EPSILON = 1e-05
MESH = pl.DeviceIdType.MESH
TILE = 48


def plan(extents):
    segments = []
    for index, extent in enumerate(extents):
        pitch = -(-(extent + 1) // 16) * 16
        if segments and segments[-1]["pitch"] == pitch:
            segments[-1]["levels"].append(index)
        else:
            segments.append({"pitch": pitch, "levels": [index]})
    base = 0
    places = {}
    for number, segment in enumerate(segments):
        pitch = segment["pitch"]
        at = 0
        holes = [(0, pitch)]
        for index in segment["levels"]:
            size = extents[index] * pitch
            places[index] = (number, at, size, pitch)
            holes.append((pitch + at + size, pitch))
            at += size + pitch
        rows = -(-(at - pitch) // 128) * 128
        last = holes.pop()
        holes.append((last[0], rows + 2 * pitch - last[0]))
        segment.update(rows=rows, base=base, holes=holes)
        base += rows
    return segments, places, base


class Hop:
    def __init__(self, size, place, target):
        self.size, self.place, self.target = size, place, target


def kernel(shape, *refs):
    names = shape["names"]
    ref = dict(zip(names, refs))
    extents, wide, group = shape["extents"], shape["wide"], shape["group"]
    segments, places, total_rows = plan(extents)
    levels = len(extents)
    ch = shape["ch"]
    w_me, g_me = lax.axis_index("wide"), lax.axis_index("group")
    x_size, y_size, z_size = shape["x"], shape["y"], shape["z"]
    devices = wide * group

    def at_group(g):
        return {"wide": w_me, "group": g}

    def at_wide(w):
        return {"wide": w, "group": g_me}

    barrier = pltpu.get_barrier_semaphore()
    for step in range(1, group):
        pl.semaphore_signal(barrier, inc=1, device_id=at_group(lax.rem(g_me + step, group)), device_id_type=MESH)
    for step in range(1, wide):
        pl.semaphore_signal(barrier, inc=1, device_id=at_wide(lax.rem(w_me + step, wide)), device_id_type=MESH)

    height, width = ref["heights"][0], ref["widths"][0]
    row_limits, col_limits = [], []
    for index in range(levels):
        stride = 16 * 2**index
        row_limits.append(jnp.minimum((height + (stride - 1)) // stride, extents[index]))
        col_limits.append(jnp.minimum((width + (stride - 1)) // stride, extents[index]))

    masks, conv = ref["masks"], ref["conv"]
    xbs = [ref[f"xb{n}"] for n in range(len(segments))]
    bbs = [ref[f"bb{n}"] for n in range(len(segments))]
    for number, segment in enumerate(segments):
        for start, count in segment["holes"]:
            xbs[number][start : start + count, :] = jnp.zeros((count, 3 * ch), jnp.bfloat16)
            bbs[number][start : start + count, :] = jnp.zeros((count, 3 * ch), jnp.bfloat16)

    def spread(target, index, values):
        number, at, size, pitch = places[index]
        rows = slice(pitch + at, pitch + at + size)
        target[number][rows, 0:ch] = pltpu.roll(values, 1, 0).astype(jnp.bfloat16)
        target[number][rows, ch : 2 * ch] = values.astype(jnp.bfloat16)
        target[number][rows, 2 * ch : 3 * ch] = pltpu.roll(values, size - 1, 0).astype(jnp.bfloat16)

    def span(index):
        number, at, size, pitch = places[index]
        start = segments[number]["base"] + at
        return start, size

    for index in range(levels):
        number, at, size, pitch = places[index]
        start, _ = span(index)
        extent = extents[index]
        spot = lax.broadcasted_iota(jnp.int32, (extent, pitch, ch), 1)
        line = lax.broadcasted_iota(jnp.int32, (extent, pitch, ch), 0)
        inside = jnp.logical_and(line < row_limits[index], spot < col_limits[index])
        mask = jnp.where(inside, 1.0, 0.0).reshape(size, ch)
        masks[start : start + size, :] = mask
        stage = ref[f"stage{index}"]
        stage[...] = jnp.zeros(stage.shape, jnp.float32)
        stage[:, 0:extent, :] = ref[f"feat{index}"][0].astype(jnp.float32)
        spread(xbs, index, stage[...].reshape(size, ch) * mask)

    weight = ref["weight"]
    sums = ref["sums1"]

    def fold(values):
        return jnp.sum(values.reshape(-1, 8, ch), axis=0)

    for number, segment in enumerate(segments):
        rows, pitch, base = segment["rows"], segment["pitch"], segment["base"]
        total = None
        for tap in range(3):
            part = jnp.dot(
                xbs[number][tap * pitch : tap * pitch + rows, :],
                weight[tap].reshape(3 * ch, ch),
                preferred_element_type=jnp.float32,
            )
            total = part if total is None else total + part
        conv[base : base + rows, :] = total
    for index in range(levels):
        start, size = span(index)
        total = jnp.zeros((8, ch), jnp.float32)
        square = jnp.zeros((8, ch), jnp.float32)
        for row in range(start, start + size, TILE):
            values = conv[row : row + TILE, :]
            masked = values * masks[row : row + TILE, :]
            total += fold(masked)
            square += fold(masked * values)
        sums[index : index + 1, 0:ch] = jnp.sum(total, axis=0, keepdims=True)
        sums[levels + index : levels + index + 1, 0:ch] = jnp.sum(square, axis=0, keepdims=True)
        cells = (row_limits[index] * col_limits[index]).astype(jnp.float32)
        for row in (index, levels + index):
            sums[row : row + 1, ch : ch + 128] = jnp.full((1, 128), cells, jnp.float32)

    pl.semaphore_wait(barrier, group - 1 + wide - 1)

    def exchange(tag, during):
        sent, first, held, second = ref["sums" + tag], ref["near" + tag], ref["held" + tag], ref["far" + tag]
        copies = []
        for step in range(1, group):
            copies.append(
                pltpu.make_async_remote_copy(
                    src_ref=sent,
                    dst_ref=first.at[g_me],
                    send_sem=ref["near_send" + tag].at[step - 1],
                    recv_sem=ref["near_recv" + tag].at[step - 1],
                    device_id=at_group(lax.rem(g_me + step, group)),
                    device_id_type=MESH,
                )
            )
            copies[-1].start()
        during[0]()
        own = sent[...]
        for copy in copies:
            copy.wait()
        total = None
        for source in range(group):
            term = jnp.where(source == g_me, own, first[source])
            total = term if total is None else total + term
        held[...] = total
        copies = []
        for step in range(1, wide):
            copies.append(
                pltpu.make_async_remote_copy(
                    src_ref=held,
                    dst_ref=second.at[w_me],
                    send_sem=ref["far_send" + tag].at[step - 1],
                    recv_sem=ref["far_recv" + tag].at[step - 1],
                    device_id=at_wide(lax.rem(w_me + step, wide)),
                    device_id_type=MESH,
                )
            )
            copies[-1].start()
        during[1]()
        own = held[...]
        for copy in copies:
            copy.wait()
        total = None
        for source in range(wide):
            term = jnp.where(source == w_me, own, second[source])
            total = term if total is None else total + term
        return total

    grads = ref["grads"]

    def take_grads():
        for index in range(levels):
            start, size = span(index)
            extent = extents[index]
            stage = ref[f"stage{index}"]
            stage[:, 0:extent, :] = ref[f"grad{index}"][0].astype(jnp.float32)
            grads[start : start + size, :] = stage[...].reshape(size, ch) * masks[start : start + size, :]

    def turn():
        for number, segment in enumerate(segments):
            rows, pitch, base = segment["rows"], segment["pitch"], segment["base"]
            for row in range(0, rows, 128):
                block = xbs[number][pitch + row : pitch + row + 128, ch : 2 * ch]
                ref["turned"][:, base + row : base + row + 128] = block.astype(jnp.float32).T.astype(jnp.bfloat16)

    moments = exchange("1", (take_grads, turn))

    sums = ref["sums2"]
    scales, counts = [], []
    for index in range(levels):
        start, size = span(index)
        count = jnp.concatenate([moments[index : index + 1, ch : ch + 128]] * (ch // 128), axis=1)
        mean = moments[index : index + 1, 0:ch] / count
        variance = jnp.maximum(moments[levels + index : levels + index + 1, 0:ch] / count - mean * mean, 0.0)
        inverse = lax.rsqrt(variance + EPSILON)
        gain = ref["gain"][index : index + 1, :]
        shift = ref["shift"][index : index + 1, :]
        counts.append(count)
        scales.append(gain * inverse)
        shift_sum = jnp.zeros((8, ch), jnp.float32)
        gain_sum = jnp.zeros((8, ch), jnp.float32)
        for row in range(start, start + size, TILE):
            normed = (conv[row : row + TILE, :] - mean) * inverse
            shifted = gain * normed + shift
            sigma = 1.0 / (1.0 + jnp.exp(-shifted))
            slope = grads[row : row + TILE, :] * sigma * (1.0 + shifted * (1.0 - sigma))
            conv[row : row + TILE, :] = normed
            grads[row : row + TILE, :] = slope
            ref["acts"][row : row + TILE, :] = masks[row : row + TILE, :] * shifted * sigma
            shift_sum += fold(slope)
            gain_sum += fold(slope * normed)
        sums[index : index + 1, :] = jnp.sum(shift_sum, axis=0, keepdims=True)
        sums[levels + index : levels + index + 1, :] = jnp.sum(gain_sum, axis=0, keepdims=True)

    def put_acts():
        for index in range(levels):
            start, size = span(index)
            extent, pitch = extents[index], places[index][3]
            values = ref["acts"][start : start + size, :].reshape(extent, pitch, ch)
            ref[f"out{index}"][0] = values[:, 0:extent, :].astype(jnp.bfloat16)

    slopes = exchange("2", (lambda: None, put_acts))
    ref["d_shift"][...] = slopes[0:levels, :] / devices
    ref["d_gain"][...] = slopes[levels : 2 * levels, :] / devices

    for index in range(levels):
        start, size = span(index)
        shift_term = slopes[index : index + 1, :] / counts[index]
        gain_term = slopes[levels + index : levels + index + 1, :] / counts[index]
        for row in range(start, start + size, TILE):
            grads[row : row + TILE, :] = (
                masks[row : row + TILE, :]
                * scales[index]
                * (grads[row : row + TILE, :] - shift_term - conv[row : row + TILE, :] * gain_term)
            )
        spread(bbs, index, grads[start : start + size, :])

    def weight_grad(tap):
        a, b = divmod(tap, 3)
        total = None
        for number, segment in enumerate(segments):
            rows, pitch, base = segment["rows"], segment["pitch"], segment["base"]
            part = jnp.dot(
                ref["turned"][:, base : base + rows],
                bbs[number][(2 - a) * pitch : (2 - a) * pitch + rows, (2 - b) * ch : (3 - b) * ch],
                preferred_element_type=jnp.float32,
            )
            total = part if total is None else total + part
        return total

    def input_grad(number, begin, count):
        pitch, base = segments[number]["pitch"], segments[number]["base"]
        total = None
        for a in range(3):
            for b in range(3):
                first = (2 - a) * pitch + begin
                part = lax.dot_general(
                    bbs[number][first : first + count, (2 - b) * ch : (3 - b) * ch],
                    weight[a, b],
                    (((1,), (1,)), ((), ())),
                    preferred_element_type=jnp.float32,
                )
                total = part if total is None else total + part
        where = slice(base + begin, base + begin + count)
        ref["acts"][where, :] = total * masks[where, :]

    def put_input_grads():
        for index in range(levels):
            start, size = span(index)
            extent, pitch = extents[index], places[index][3]
            values = ref["acts"][start : start + size, :].reshape(extent, pitch, ch)
            ref[f"d_feat{index}"][0] = values[:, 0:extent, :].astype(jnp.bfloat16)

    jobs = []
    for number, segment in enumerate(segments):
        tall = 256 if segment["rows"] % 256 == 0 else segment["rows"]
        for begin in range(0, segment["rows"], tall):
            jobs.append(functools.partial(input_grad, number, begin, tall))
    jobs.append(put_input_grads)

    if not shape["fused"]:
        for tap in range(9):
            ref["d_weight"][tap] = weight_grad(tap)
        for job in jobs:
            job()
        return

    part_ref, whole = ref["parts"], ref["d_weight"]
    core, y_me = lax.rem(g_me, 2), g_me // 2
    z_me, x_me = w_me // x_size, lax.rem(w_me, x_size)
    hops = {
        "core": Hop(2, core, lambda k: at_group(y_me * 2 + k)),
        "y": Hop(y_size, y_me, lambda k: at_group(k * 2 + core)),
        "x": Hop(x_size, x_me, lambda k: at_wide(z_me * x_size + k)),
        "z": Hop(z_size, z_me, lambda k: at_wide(k * x_size + x_me)),
    }

    class Chunk:
        def __init__(self, tap):
            self.tap = tap
            order = ("core", "x", "y", "z") if tap % 2 == 0 else ("core", "y", "x", "z")
            self.hops = [hops[name] for name in order]
            self.offsets, self.sizes = [0], [ch]
            for hop in self.hops:
                self.sizes.append(self.sizes[-1] // hop.size)
                self.offsets.append(self.offsets[-1] + hop.place * self.sizes[-1])
            self.flying = None

        def rows(self, offset, count):
            return pl.ds(pl.multiple_of(offset, 8), count)

        def sems(self, kind, level, step):
            before = sum(hop.size - 1 for hop in self.hops[:level]) + step - 1
            return ref[kind + "_send"].at[self.tap, before], ref[kind + "_recv"].at[self.tap, before]

        def scatter(self, level):
            hop, size = self.hops[level], self.sizes[level + 1]
            self.flying = []
            for step in range(1, hop.size):
                peer = lax.rem(hop.place + step, hop.size)
                send, recv = self.sems("rs", level, step)
                copy = pltpu.make_async_remote_copy(
                    src_ref=part_ref.at[self.tap, self.rows(self.offsets[level] + peer * size, size), :],
                    dst_ref=ref[f"land{level}"].at[self.tap, pl.ds((step - 1) * size, size), :],
                    send_sem=send,
                    recv_sem=recv,
                    device_id=hop.target(peer),
                    device_id_type=MESH,
                )
                copy.start()
                self.flying.append(copy)

        def gather(self, level):
            hop, size = self.hops[level], self.sizes[level + 1]
            mine = whole.at[self.tap, self.rows(self.offsets[level + 1], size), :]
            self.flying = []
            for step in range(1, hop.size):
                peer = lax.rem(hop.place + step, hop.size)
                send, recv = self.sems("ag", level, step)
                copy = pltpu.make_async_remote_copy(
                    src_ref=mine, dst_ref=mine, send_sem=send, recv_sem=recv,
                    device_id=hop.target(peer), device_id_type=MESH,
                )
                copy.start()
                self.flying.append(copy)

        def step(self, number):
            count = len(self.hops)
            if number == 0:
                part_ref[self.tap] = weight_grad(self.tap)
                self.scatter(0)
            elif number <= count:
                for copy in self.flying:
                    copy.wait()
                size = self.sizes[number]
                where = self.rows(self.offsets[number], size)
                total = part_ref[self.tap, where, :]
                for slot in range(self.hops[number - 1].size - 1):
                    total = total + ref[f"land{number - 1}"][self.tap, slot * size : (slot + 1) * size, :]
                if number < count:
                    part_ref[self.tap, where, :] = total
                    self.scatter(number)
                else:
                    whole[self.tap, where, :] = total
                    self.gather(count - 1)
            else:
                for copy in self.flying:
                    copy.wait()
                if number < 2 * count:
                    self.gather(2 * count - 1 - number)

    chunks = [Chunk(tap) for tap in range(9)]
    for tap in range(9 + 2):
        if tap < 9:
            chunks[tap].step(0)
        if tap >= 2:
            chunks[tap - 2].step(1)
    last = 2 * 4
    for wave in range(9 + last):
        if jobs:
            jobs.pop(0)()
        for tap in range(9):
            number = 2 + wave - tap
            if 2 <= number <= last:
                chunks[tap].step(number)
    for job in jobs:
        job()


def shards(mesh_shape, *arrays):
    feats, cots = arrays[0:4], arrays[4:8]
    weight, gain, shift, heights, widths = arrays[8:13]
    wide, group = mesh_shape["wide"], mesh_shape["group"]
    extents = tuple(feat.shape[1] for feat in feats)
    ch = weight.shape[3]
    devices = wide * group
    y_size = max(group // 2, 1)
    x_size = math.gcd(y_size, wide)
    z_size = wide // x_size
    fused = group == 2 * y_size and ch % (8 * devices) == 0
    segments, places, total_rows = plan(extents)
    levels = len(extents)
    vmem = pl.BlockSpec(memory_space=pltpu.VMEM)
    smem = pl.BlockSpec(memory_space=pltpu.SMEM)

    names, ins = [], []

    def give(name, array, spec):
        names.append(name)
        ins.append((array, spec))

    for index in range(levels):
        give(f"feat{index}", feats[index], vmem)
    for index in range(levels):
        give(f"grad{index}", cots[index], vmem)
    give("weight", weight, vmem)
    give("gain", gain, vmem)
    give("shift", shift, vmem)
    give("heights", heights, smem)
    give("widths", widths, smem)

    outs = []
    for index in range(levels):
        names.append(f"out{index}")
        outs.append(jax.ShapeDtypeStruct(feats[index].shape, jnp.bfloat16))
    for index in range(levels):
        names.append(f"d_feat{index}")
        outs.append(jax.ShapeDtypeStruct(feats[index].shape, jnp.bfloat16))
    names.append("d_weight")
    outs.append(jax.ShapeDtypeStruct((9, ch, ch), jnp.float32))
    for name in ("d_gain", "d_shift"):
        names.append(name)
        outs.append(jax.ShapeDtypeStruct((levels, ch), jnp.float32))

    scratch = []

    def hold(name, kind):
        names.append(name)
        scratch.append(kind)

    f32 = jnp.float32
    for number, segment in enumerate(segments):
        tall = segment["rows"] + 2 * segment["pitch"]
        hold(f"xb{number}", pltpu.VMEM((tall, 3 * ch), jnp.bfloat16))
        hold(f"bb{number}", pltpu.VMEM((tall, 3 * ch), jnp.bfloat16))
    for index in range(levels):
        hold(f"stage{index}", pltpu.VMEM((extents[index], places[index][3], ch), f32))
    for name in ("masks", "conv", "grads", "acts"):
        hold(name, pltpu.VMEM((total_rows, ch), f32))
    hold("turned", pltpu.VMEM((ch, total_rows), jnp.bfloat16))
    for tag, across in (("1", ch + 128), ("2", ch)):
        hold("sums" + tag, pltpu.VMEM((2 * levels, across), f32))
        hold("held" + tag, pltpu.VMEM((2 * levels, across), f32))
        hold("near" + tag, pltpu.VMEM((group, 2 * levels, across), f32))
        hold("far" + tag, pltpu.VMEM((wide, 2 * levels, across), f32))
        for name, size in (("near", group), ("far", wide)):
            hold(f"{name}_send{tag}", pltpu.SemaphoreType.DMA((max(size - 1, 1),)))
            hold(f"{name}_recv{tag}", pltpu.SemaphoreType.DMA((max(size - 1, 1),)))
    if fused:
        hold("parts", pltpu.VMEM((9, ch, ch), f32))
        hold("land0", pltpu.VMEM((9, ch // 2, ch), f32))
        across = x_size
        rows = ch // 2
        hold("land1", pltpu.VMEM((9, rows // x_size * (x_size - 1), ch), f32))
        rows //= x_size
        hold("land2", pltpu.VMEM((9, rows // y_size * (y_size - 1), ch), f32))
        rows //= y_size
        hold("land3", pltpu.VMEM((9, rows // z_size * (z_size - 1), ch), f32))
        flights = 1 + x_size - 1 + y_size - 1 + z_size - 1
        for name in ("rs_send", "rs_recv", "ag_send", "ag_recv"):
            hold(name, pltpu.SemaphoreType.DMA((9, flights)))

    shape = dict(
        names=names, extents=extents, wide=wide, group=group, ch=ch,
        x=x_size, y=y_size, z=z_size, fused=fused,
    )
    results = pl.pallas_call(
        functools.partial(kernel, shape),
        out_shape=outs,
        in_specs=[spec for _, spec in ins],
        out_specs=[vmem] * len(outs),
        scratch_shapes=scratch,
        compiler_params=pltpu.CompilerParams(
            collective_id=0, has_side_effects=True, vmem_limit_bytes=58 * 1024 * 1024
        ),
    )(*[array for array, _ in ins])
    results = list(results)
    d_weight = results[2 * levels]
    if not fused:
        d_weight = lax.psum(d_weight, ("wide", "group"))
    results[2 * levels] = (d_weight / devices).reshape(weight.shape)
    return tuple(results)


def solution(mesh):
    image = P(("wide", "group"), None, None, None)
    return jax.shard_map(
        functools.partial(shards, dict(mesh.shape)),
        mesh=mesh,
        in_specs=(image,) * 8 + (P(),) * 3 + (P(("wide", "group")),) * 2,
        out_specs=(image,) * 8 + (P(),) * 3,
        check_vma=False,
    )
```

```python
import functools
import math

import jax
import jax.numpy as jnp
from jax import lax
from jax.experimental import pallas as pl
from jax.experimental.pallas import tpu as pltpu
from jax.sharding import PartitionSpec as P

EPSILON = 1e-05
MESH = pl.DeviceIdType.MESH
TILE = 48
SKEW = 3


def plan(extents):
    segments = []
    for index, extent in enumerate(extents):
        pitch = -(-(extent + 1) // 16) * 16
        if segments and segments[-1]["pitch"] == pitch:
            segments[-1]["levels"].append(index)
        else:
            segments.append({"pitch": pitch, "levels": [index]})
    base = 0
    places = {}
    for number, segment in enumerate(segments):
        pitch = segment["pitch"]
        at = 0
        holes = [(0, pitch)]
        for index in segment["levels"]:
            size = extents[index] * pitch
            places[index] = (number, at, size, pitch)
            holes.append((pitch + at + size, pitch))
            at += size + pitch
        rows = -(-(at - pitch) // 128) * 128
        last = holes.pop()
        holes.append((last[0], rows + 2 * pitch - last[0]))
        segment.update(rows=rows, base=base, holes=holes)
        base += rows
    return segments, places, base


class Hop:
    def __init__(self, size, place, target):
        self.size, self.place, self.target = size, place, target


def kernel(shape, *refs):
    names = shape["names"]
    ref = dict(zip(names, refs))
    extents, wide, group = shape["extents"], shape["wide"], shape["group"]
    segments, places, total_rows = plan(extents)
    levels = len(extents)
    ch = shape["ch"]
    w_me, g_me = lax.axis_index("wide"), lax.axis_index("group")
    x_size, y_size, z_size = shape["x"], shape["y"], shape["z"]
    devices = wide * group

    def at_group(g):
        return {"wide": w_me, "group": g}

    def at_wide(w):
        return {"wide": w, "group": g_me}

    barrier = pltpu.get_barrier_semaphore()
    for step in range(1, group):
        pl.semaphore_signal(barrier, inc=1, device_id=at_group(lax.rem(g_me + step, group)), device_id_type=MESH)
    for step in range(1, wide):
        pl.semaphore_signal(barrier, inc=1, device_id=at_wide(lax.rem(w_me + step, wide)), device_id_type=MESH)

    height, width = ref["heights"][0], ref["widths"][0]
    row_limits, col_limits = [], []
    for index in range(levels):
        stride = 16 * 2**index
        row_limits.append(jnp.minimum((height + (stride - 1)) // stride, extents[index]))
        col_limits.append(jnp.minimum((width + (stride - 1)) // stride, extents[index]))

    masks, conv = ref["masks"], ref["conv"]
    xbs = [ref[f"xb{n}"] for n in range(len(segments))]
    bbs = [ref[f"bb{n}"] for n in range(len(segments))]
    for number, segment in enumerate(segments):
        for start, count in segment["holes"]:
            xbs[number][start : start + count, :] = jnp.zeros((count, 3 * ch), jnp.bfloat16)
            bbs[number][start : start + count, :] = jnp.zeros((count, 3 * ch), jnp.bfloat16)

    def spread(target, index, values):
        number, at, size, pitch = places[index]
        rows = slice(pitch + at, pitch + at + size)
        target[number][rows, 0:ch] = pltpu.roll(values, 1, 0).astype(jnp.bfloat16)
        target[number][rows, ch : 2 * ch] = values.astype(jnp.bfloat16)
        target[number][rows, 2 * ch : 3 * ch] = pltpu.roll(values, size - 1, 0).astype(jnp.bfloat16)

    def span(index):
        number, at, size, pitch = places[index]
        start = segments[number]["base"] + at
        return start, size

    for index in range(levels):
        number, at, size, pitch = places[index]
        start, _ = span(index)
        extent = extents[index]
        spot = lax.broadcasted_iota(jnp.int32, (extent, pitch, ch), 1)
        line = lax.broadcasted_iota(jnp.int32, (extent, pitch, ch), 0)
        inside = jnp.logical_and(line < row_limits[index], spot < col_limits[index])
        mask = jnp.where(inside, 1.0, 0.0).reshape(size, ch)
        masks[start : start + size, :] = mask
        stage = ref[f"stage{index}"]
        stage[...] = jnp.zeros(stage.shape, jnp.float32)
        stage[:, 0:extent, :] = ref[f"feat{index}"][0].astype(jnp.float32)
        spread(xbs, index, stage[...].reshape(size, ch) * mask)

    weight = ref["weight"]
    sums = ref["sums1"]

    def fold(values):
        return jnp.sum(values.reshape(-1, 8, ch), axis=0)

    for number, segment in enumerate(segments):
        rows, pitch, base = segment["rows"], segment["pitch"], segment["base"]
        total = None
        for tap in range(3):
            part = jnp.dot(
                xbs[number][tap * pitch : tap * pitch + rows, :],
                weight[tap].reshape(3 * ch, ch),
                preferred_element_type=jnp.float32,
            )
            total = part if total is None else total + part
        conv[base : base + rows, :] = total
    for index in range(levels):
        start, size = span(index)
        total = jnp.zeros((8, ch), jnp.float32)
        square = jnp.zeros((8, ch), jnp.float32)
        for row in range(start, start + size, TILE):
            values = conv[row : row + TILE, :]
            masked = values * masks[row : row + TILE, :]
            total += fold(masked)
            square += fold(masked * values)
        sums[index : index + 1, 0:ch] = jnp.sum(total, axis=0, keepdims=True)
        sums[levels + index : levels + index + 1, 0:ch] = jnp.sum(square, axis=0, keepdims=True)
        cells = (row_limits[index] * col_limits[index]).astype(jnp.float32)
        for row in (index, levels + index):
            sums[row : row + 1, ch : ch + 128] = jnp.full((1, 128), cells, jnp.float32)

    pl.semaphore_wait(barrier, group - 1 + wide - 1)

    def exchange(tag, during):
        sent, first, held, second = ref["sums" + tag], ref["near" + tag], ref["held" + tag], ref["far" + tag]
        copies = []
        for step in range(1, group):
            copies.append(
                pltpu.make_async_remote_copy(
                    src_ref=sent,
                    dst_ref=first.at[g_me],
                    send_sem=ref["near_send" + tag].at[step - 1],
                    recv_sem=ref["near_recv" + tag].at[step - 1],
                    device_id=at_group(lax.rem(g_me + step, group)),
                    device_id_type=MESH,
                )
            )
            copies[-1].start()
        during[0]()
        own = sent[...]
        for copy in copies:
            copy.wait()
        total = None
        for source in range(group):
            term = jnp.where(source == g_me, own, first[source])
            total = term if total is None else total + term
        held[...] = total
        copies = []
        for step in range(1, wide):
            copies.append(
                pltpu.make_async_remote_copy(
                    src_ref=held,
                    dst_ref=second.at[w_me],
                    send_sem=ref["far_send" + tag].at[step - 1],
                    recv_sem=ref["far_recv" + tag].at[step - 1],
                    device_id=at_wide(lax.rem(w_me + step, wide)),
                    device_id_type=MESH,
                )
            )
            copies[-1].start()
        during[1]()
        own = held[...]
        for copy in copies:
            copy.wait()
        total = None
        for source in range(wide):
            term = jnp.where(source == w_me, own, second[source])
            total = term if total is None else total + term
        return total

    grads = ref["grads"]

    def take_grads():
        for index in range(levels):
            start, size = span(index)
            extent = extents[index]
            stage = ref[f"stage{index}"]
            stage[:, 0:extent, :] = ref[f"grad{index}"][0].astype(jnp.float32)
            grads[start : start + size, :] = stage[...].reshape(size, ch) * masks[start : start + size, :]

    def turn():
        for number, segment in enumerate(segments):
            rows, pitch, base = segment["rows"], segment["pitch"], segment["base"]
            for row in range(0, rows, 128):
                block = xbs[number][pitch + row : pitch + row + 128, ch : 2 * ch]
                ref["turned"][:, base + row : base + row + 128] = block.astype(jnp.float32).T.astype(jnp.bfloat16)

    moments = exchange("1", (take_grads, turn))

    sums = ref["sums2"]
    scales, counts = [], []
    for index in range(levels):
        start, size = span(index)
        count = jnp.concatenate([moments[index : index + 1, ch : ch + 128]] * (ch // 128), axis=1)
        mean = moments[index : index + 1, 0:ch] / count
        variance = jnp.maximum(moments[levels + index : levels + index + 1, 0:ch] / count - mean * mean, 0.0)
        inverse = lax.rsqrt(variance + EPSILON)
        gain = ref["gain"][index : index + 1, :]
        shift = ref["shift"][index : index + 1, :]
        counts.append(count)
        scales.append(gain * inverse)
        shift_sum = jnp.zeros((8, ch), jnp.float32)
        gain_sum = jnp.zeros((8, ch), jnp.float32)
        for row in range(start, start + size, TILE):
            normed = (conv[row : row + TILE, :] - mean) * inverse
            shifted = gain * normed + shift
            sigma = 1.0 / (1.0 + jnp.exp(-shifted))
            slope = grads[row : row + TILE, :] * sigma * (1.0 + shifted * (1.0 - sigma))
            conv[row : row + TILE, :] = normed
            grads[row : row + TILE, :] = slope
            ref["acts"][row : row + TILE, :] = masks[row : row + TILE, :] * shifted * sigma
            shift_sum += fold(slope)
            gain_sum += fold(slope * normed)
        sums[index : index + 1, :] = jnp.sum(shift_sum, axis=0, keepdims=True)
        sums[levels + index : levels + index + 1, :] = jnp.sum(gain_sum, axis=0, keepdims=True)

    def put_acts():
        for index in range(levels):
            start, size = span(index)
            extent, pitch = extents[index], places[index][3]
            values = ref["acts"][start : start + size, :].reshape(extent, pitch, ch)
            ref[f"out{index}"][0] = values[:, 0:extent, :].astype(jnp.bfloat16)

    slopes = exchange("2", (lambda: None, put_acts))
    ref["d_shift"][...] = slopes[0:levels, :] / devices
    ref["d_gain"][...] = slopes[levels : 2 * levels, :] / devices

    for index in range(levels):
        start, size = span(index)
        shift_term = slopes[index : index + 1, :] / counts[index]
        gain_term = slopes[levels + index : levels + index + 1, :] / counts[index]
        for row in range(start, start + size, TILE):
            grads[row : row + TILE, :] = (
                masks[row : row + TILE, :]
                * scales[index]
                * (grads[row : row + TILE, :] - shift_term - conv[row : row + TILE, :] * gain_term)
            )
        spread(bbs, index, grads[start : start + size, :])

    def weight_grad(tap):
        a, b = divmod(tap, 3)
        total = None
        for number, segment in enumerate(segments):
            rows, pitch, base = segment["rows"], segment["pitch"], segment["base"]
            part = jnp.dot(
                ref["turned"][:, base : base + rows],
                bbs[number][(2 - a) * pitch : (2 - a) * pitch + rows, (2 - b) * ch : (3 - b) * ch],
                preferred_element_type=jnp.float32,
            )
            total = part if total is None else total + part
        return total

    def input_grad(number, begin, count):
        pitch, base = segments[number]["pitch"], segments[number]["base"]
        total = None
        for a in range(3):
            for b in range(3):
                first = (2 - a) * pitch + begin
                part = lax.dot_general(
                    bbs[number][first : first + count, (2 - b) * ch : (3 - b) * ch],
                    weight[a, b],
                    (((1,), (1,)), ((), ())),
                    preferred_element_type=jnp.float32,
                )
                total = part if total is None else total + part
        where = slice(base + begin, base + begin + count)
        ref["acts"][where, :] = total * masks[where, :]

    def put_input_grads():
        for index in range(levels):
            start, size = span(index)
            extent, pitch = extents[index], places[index][3]
            values = ref["acts"][start : start + size, :].reshape(extent, pitch, ch)
            ref[f"d_feat{index}"][0] = values[:, 0:extent, :].astype(jnp.bfloat16)

    jobs = []
    for number, segment in enumerate(segments):
        tall = 256 if segment["rows"] % 256 == 0 else segment["rows"]
        for begin in range(0, segment["rows"], tall):
            jobs.append(functools.partial(input_grad, number, begin, tall))
    jobs.append(put_input_grads)

    if not shape["fused"]:
        for tap in range(9):
            ref["d_weight"][tap] = weight_grad(tap)
        for job in jobs:
            job()
        return

    part_ref, whole = ref["parts"], ref["d_weight"]
    core, y_me = lax.rem(g_me, 2), g_me // 2
    z_me, x_me = w_me // x_size, lax.rem(w_me, x_size)
    hops = {
        "core": Hop(2, core, lambda k: at_group(y_me * 2 + k)),
        "y": Hop(y_size, y_me, lambda k: at_group(k * 2 + core)),
        "x": Hop(x_size, x_me, lambda k: at_wide(z_me * x_size + k)),
        "z": Hop(z_size, z_me, lambda k: at_wide(k * x_size + x_me)),
    }

    class Chunk:
        def __init__(self, tap):
            self.tap = tap
            order = ("core", "x", "y", "z") if tap % 2 == 0 else ("core", "y", "x", "z")
            self.hops = [hops[name] for name in order]
            self.offsets, self.sizes = [0], [ch]
            for hop in self.hops:
                self.sizes.append(self.sizes[-1] // hop.size)
                self.offsets.append(self.offsets[-1] + hop.place * self.sizes[-1])
            self.flying = None

        def rows(self, offset, count):
            return pl.ds(pl.multiple_of(offset, 8), count)

        def sems(self, kind, level, step):
            before = sum(hop.size - 1 for hop in self.hops[:level]) + step - 1
            return ref[kind + "_send"].at[self.tap, before], ref[kind + "_recv"].at[self.tap, before]

        def scatter(self, level):
            hop, size = self.hops[level], self.sizes[level + 1]
            self.flying = []
            for step in range(1, hop.size):
                peer = lax.rem(hop.place + step, hop.size)
                send, recv = self.sems("rs", level, step)
                copy = pltpu.make_async_remote_copy(
                    src_ref=part_ref.at[self.tap, self.rows(self.offsets[level] + peer * size, size), :],
                    dst_ref=ref[f"land{level}"].at[self.tap, pl.ds((step - 1) * size, size), :],
                    send_sem=send,
                    recv_sem=recv,
                    device_id=hop.target(peer),
                    device_id_type=MESH,
                )
                copy.start()
                self.flying.append(copy)

        def gather(self, level):
            hop, size = self.hops[level], self.sizes[level + 1]
            mine = whole.at[self.tap, self.rows(self.offsets[level + 1], size), :]
            self.flying = []
            for step in range(1, hop.size):
                peer = lax.rem(hop.place + step, hop.size)
                send, recv = self.sems("ag", level, step)
                copy = pltpu.make_async_remote_copy(
                    src_ref=mine, dst_ref=mine, send_sem=send, recv_sem=recv,
                    device_id=hop.target(peer), device_id_type=MESH,
                )
                copy.start()
                self.flying.append(copy)

        def step(self, number):
            count = len(self.hops)
            if number == 0:
                part_ref[self.tap] = weight_grad(self.tap)
                self.scatter(0)
            elif number <= count:
                for copy in self.flying:
                    copy.wait()
                size = self.sizes[number]
                where = self.rows(self.offsets[number], size)
                total = part_ref[self.tap, where, :]
                for slot in range(self.hops[number - 1].size - 1):
                    total = total + ref[f"land{number - 1}"][self.tap, slot * size : (slot + 1) * size, :]
                if number < count:
                    part_ref[self.tap, where, :] = total
                    self.scatter(number)
                else:
                    whole[self.tap, where, :] = total / devices
                    self.gather(count - 1)
            else:
                for copy in self.flying:
                    copy.wait()
                if number < 2 * count:
                    self.gather(2 * count - 1 - number)

    chunks = [Chunk(tap) for tap in range(9)]
    for tap in range(9 + 2):
        if tap < 9:
            chunks[tap].step(0)
        if tap >= 2:
            chunks[tap - 2].step(1)
    turns = [(tap + SKEW * number, -number, tap) for tap in range(9) for number in range(2, 9)]
    for place, (_, number, tap) in enumerate(sorted(turns)):
        if jobs and place % 2 == 0:
            jobs.pop(0)()
        chunks[tap].step(-number)


def hand_on(arrays):
    count = len(arrays)

    def body(*refs):
        sources, targets, held = refs[:count], refs[count : 2 * count], refs[2 * count : 3 * count]
        read, write = refs[3 * count :]
        reads = [pltpu.make_async_copy(sources[i], held[i], read.at[i]) for i in range(count)]
        writes = [pltpu.make_async_copy(held[i], targets[i], write.at[i]) for i in range(count)]
        for copy in reads:
            copy.start()
        for first, second in zip(reads, writes):
            first.wait()
            second.start()
        for copy in writes:
            copy.wait()

    return list(
        pl.pallas_call(
            body,
            out_shape=[jax.ShapeDtypeStruct(array.shape, array.dtype) for array in arrays],
            in_specs=[pl.BlockSpec(memory_space=pl.ANY)] * count,
            out_specs=[pl.BlockSpec(memory_space=pl.ANY)] * count,
            scratch_shapes=[pltpu.VMEM(array.shape, array.dtype) for array in arrays]
            + [pltpu.SemaphoreType.DMA((count,))] * 2,
            compiler_params=pltpu.CompilerParams(vmem_limit_bytes=8 * 1024 * 1024),
        )(*arrays)
    )


def shards(mesh_shape, *arrays):
    feats, cots = arrays[0:4], arrays[4:8]
    weight, gain, shift, heights, widths = arrays[8:13]
    wide, group = mesh_shape["wide"], mesh_shape["group"]
    extents = tuple(feat.shape[1] for feat in feats)
    ch = weight.shape[3]
    devices = wide * group
    y_size = max(group // 2, 1)
    x_size = math.gcd(y_size, wide)
    z_size = wide // x_size
    fused = group == 2 * y_size and ch % (8 * devices) == 0
    segments, places, total_rows = plan(extents)
    levels = len(extents)
    vmem = pl.BlockSpec(memory_space=pltpu.VMEM)
    smem = pl.BlockSpec(memory_space=pltpu.SMEM)

    names, ins = [], []

    def give(name, array, spec):
        names.append(name)
        ins.append((array, spec))

    for index in range(levels):
        give(f"feat{index}", feats[index], vmem)
    for index in range(levels):
        give(f"grad{index}", cots[index], vmem)
    give("weight", weight, vmem)
    give("gain", gain, vmem)
    give("shift", shift, vmem)
    give("heights", heights, smem)
    give("widths", widths, smem)

    outs = []
    for index in range(levels):
        names.append(f"out{index}")
        outs.append(jax.ShapeDtypeStruct(feats[index].shape, jnp.bfloat16))
    for index in range(levels):
        names.append(f"d_feat{index}")
        outs.append(jax.ShapeDtypeStruct(feats[index].shape, jnp.bfloat16))
    names.append("d_weight")
    outs.append(jax.ShapeDtypeStruct((9, ch, ch), jnp.float32))
    for name in ("d_gain", "d_shift"):
        names.append(name)
        outs.append(jax.ShapeDtypeStruct((levels, ch), jnp.float32))

    scratch = []

    def hold(name, kind):
        names.append(name)
        scratch.append(kind)

    f32 = jnp.float32
    for number, segment in enumerate(segments):
        tall = segment["rows"] + 2 * segment["pitch"]
        hold(f"xb{number}", pltpu.VMEM((tall, 3 * ch), jnp.bfloat16))
        hold(f"bb{number}", pltpu.VMEM((tall, 3 * ch), jnp.bfloat16))
    for index in range(levels):
        hold(f"stage{index}", pltpu.VMEM((extents[index], places[index][3], ch), f32))
    for name in ("masks", "conv", "grads", "acts"):
        hold(name, pltpu.VMEM((total_rows, ch), f32))
    hold("turned", pltpu.VMEM((ch, total_rows), jnp.bfloat16))
    for tag, across in (("1", ch + 128), ("2", ch)):
        hold("sums" + tag, pltpu.VMEM((2 * levels, across), f32))
        hold("held" + tag, pltpu.VMEM((2 * levels, across), f32))
        hold("near" + tag, pltpu.VMEM((group, 2 * levels, across), f32))
        hold("far" + tag, pltpu.VMEM((wide, 2 * levels, across), f32))
        for name, size in (("near", group), ("far", wide)):
            hold(f"{name}_send{tag}", pltpu.SemaphoreType.DMA((max(size - 1, 1),)))
            hold(f"{name}_recv{tag}", pltpu.SemaphoreType.DMA((max(size - 1, 1),)))
    if fused:
        hold("parts", pltpu.VMEM((9, ch, ch), f32))
        hold("land0", pltpu.VMEM((9, ch // 2, ch), f32))
        across = x_size
        rows = ch // 2
        hold("land1", pltpu.VMEM((9, rows // x_size * (x_size - 1), ch), f32))
        rows //= x_size
        hold("land2", pltpu.VMEM((9, rows // y_size * (y_size - 1), ch), f32))
        rows //= y_size
        hold("land3", pltpu.VMEM((9, rows // z_size * (z_size - 1), ch), f32))
        flights = 1 + x_size - 1 + y_size - 1 + z_size - 1
        for name in ("rs_send", "rs_recv", "ag_send", "ag_recv"):
            hold(name, pltpu.SemaphoreType.DMA((9, flights)))

    shape = dict(
        names=names, extents=extents, wide=wide, group=group, ch=ch,
        x=x_size, y=y_size, z=z_size, fused=fused,
    )
    results = pl.pallas_call(
        functools.partial(kernel, shape),
        out_shape=outs,
        in_specs=[spec for _, spec in ins],
        out_specs=[vmem] * len(outs),
        scratch_shapes=scratch,
        compiler_params=pltpu.CompilerParams(
            collective_id=0, has_side_effects=True, vmem_limit_bytes=32 * 1024 * 1024
        ),
    )(*[array for array, _ in ins])
    results = list(results)
    d_weight = results.pop(2 * levels)
    if fused:
        *results, d_weight = hand_on(results + [d_weight])
    else:
        results = hand_on(results)
        d_weight = lax.psum(d_weight, ("wide", "group")) / devices
    results.insert(2 * levels, d_weight.reshape(weight.shape))
    return tuple(results)


def solution(mesh):
    image = P(("wide", "group"), None, None, None)
    return jax.shard_map(
        functools.partial(shards, dict(mesh.shape)),
        mesh=mesh,
        in_specs=(image,) * 8 + (P(),) * 3 + (P(("wide", "group")),) * 2,
        out_specs=(image,) * 8 + (P(),) * 3,
        check_vma=False,
    )
```

```python
import functools
import math

import jax
import jax.numpy as jnp
from jax import lax
from jax.experimental import pallas as pl
from jax.experimental.pallas import tpu as pltpu
from jax.sharding import PartitionSpec as P

EPSILON = 1e-05
MESH = pl.DeviceIdType.MESH
TILE = 48
SKEW = 3


def plan(extents):
    segments = []
    for index, extent in enumerate(extents):
        pitch = -(-(extent + 1) // 16) * 16
        if segments and segments[-1]["pitch"] == pitch:
            segments[-1]["levels"].append(index)
        else:
            segments.append({"pitch": pitch, "levels": [index]})
    base = 0
    places = {}
    for number, segment in enumerate(segments):
        pitch = segment["pitch"]
        at = 0
        holes = [(0, pitch)]
        for index in segment["levels"]:
            size = extents[index] * pitch
            places[index] = (number, at, size, pitch)
            holes.append((pitch + at + size, pitch))
            at += size + pitch
        rows = -(-(at - pitch) // 128) * 128
        last = holes.pop()
        holes.append((last[0], rows + 2 * pitch - last[0]))
        segment.update(rows=rows, base=base, holes=holes)
        base += rows
    return segments, places, base


class Hop:
    def __init__(self, size, place, target):
        self.size, self.place, self.target = size, place, target


def kernel(shape, *refs):
    names = shape["names"]
    ref = dict(zip(names, refs))
    extents, wide, group = shape["extents"], shape["wide"], shape["group"]
    segments, places, total_rows = plan(extents)
    levels = len(extents)
    ch = shape["ch"]
    w_me, g_me = lax.axis_index("wide"), lax.axis_index("group")
    x_size, y_size, z_size = shape["x"], shape["y"], shape["z"]
    devices = wide * group

    def at_group(g):
        return {"wide": w_me, "group": g}

    def at_wide(w):
        return {"wide": w, "group": g_me}

    loads = {}
    for number, name in enumerate(shape["loaded"]):
        loads[name] = pltpu.make_async_copy(ref[name], ref["vmem_" + name], ref["load"].at[number])
        loads[name].start()
        ref[name] = ref["vmem_" + name]
    stores = {}
    for number, name in enumerate(shape["stored"]):
        stores[name] = pltpu.make_async_copy(ref["vmem_" + name], ref[name], ref["store"].at[number])
        ref[name] = ref["vmem_" + name]
    barrier = pltpu.get_barrier_semaphore()
    for step in range(1, group):
        pl.semaphore_signal(barrier, inc=1, device_id=at_group(lax.rem(g_me + step, group)), device_id_type=MESH)
    for step in range(1, wide):
        pl.semaphore_signal(barrier, inc=1, device_id=at_wide(lax.rem(w_me + step, wide)), device_id_type=MESH)

    height, width = ref["heights"][0], ref["widths"][0]
    row_limits, col_limits = [], []
    for index in range(levels):
        stride = 16 * 2**index
        row_limits.append(jnp.minimum((height + (stride - 1)) // stride, extents[index]))
        col_limits.append(jnp.minimum((width + (stride - 1)) // stride, extents[index]))

    masks, conv = ref["masks"], ref["conv"]
    xbs = [ref[f"xb{n}"] for n in range(len(segments))]
    bbs = [ref[f"bb{n}"] for n in range(len(segments))]
    for number, segment in enumerate(segments):
        for start, count in segment["holes"]:
            xbs[number][start : start + count, :] = jnp.zeros((count, 3 * ch), jnp.bfloat16)
            bbs[number][start : start + count, :] = jnp.zeros((count, 3 * ch), jnp.bfloat16)

    def spread(target, index, values):
        number, at, size, pitch = places[index]
        rows = slice(pitch + at, pitch + at + size)
        target[number][rows, 0:ch] = pltpu.roll(values, 1, 0).astype(jnp.bfloat16)
        target[number][rows, ch : 2 * ch] = values.astype(jnp.bfloat16)
        target[number][rows, 2 * ch : 3 * ch] = pltpu.roll(values, size - 1, 0).astype(jnp.bfloat16)

    def span(index):
        number, at, size, pitch = places[index]
        start = segments[number]["base"] + at
        return start, size

    for index in range(levels):
        number, at, size, pitch = places[index]
        start, _ = span(index)
        extent = extents[index]
        spot = lax.broadcasted_iota(jnp.int32, (extent, pitch, ch), 1)
        line = lax.broadcasted_iota(jnp.int32, (extent, pitch, ch), 0)
        inside = jnp.logical_and(line < row_limits[index], spot < col_limits[index])
        mask = jnp.where(inside, 1.0, 0.0).reshape(size, ch)
        masks[start : start + size, :] = mask
        stage = ref[f"stage{index}"]
        stage[...] = jnp.zeros(stage.shape, jnp.float32)
        loads[f"feat{index}"].wait()
        stage[:, 0:extent, :] = ref[f"feat{index}"][0].astype(jnp.float32)
        spread(xbs, index, stage[...].reshape(size, ch) * mask)

    loads["weight"].wait()
    weight = ref["weight"]
    sums = ref["sums1"]

    def fold(values):
        return jnp.sum(values.reshape(-1, 8, ch), axis=0)

    for number, segment in enumerate(segments):
        rows, pitch, base = segment["rows"], segment["pitch"], segment["base"]
        total = None
        for tap in range(3):
            part = jnp.dot(
                xbs[number][tap * pitch : tap * pitch + rows, :],
                weight[tap].reshape(3 * ch, ch),
                preferred_element_type=jnp.float32,
            )
            total = part if total is None else total + part
        conv[base : base + rows, :] = total
    for index in range(levels):
        start, size = span(index)
        total = jnp.zeros((8, ch), jnp.float32)
        square = jnp.zeros((8, ch), jnp.float32)
        for row in range(start, start + size, TILE):
            values = conv[row : row + TILE, :]
            masked = values * masks[row : row + TILE, :]
            total += fold(masked)
            square += fold(masked * values)
        sums[index : index + 1, 0:ch] = jnp.sum(total, axis=0, keepdims=True)
        sums[levels + index : levels + index + 1, 0:ch] = jnp.sum(square, axis=0, keepdims=True)
        cells = (row_limits[index] * col_limits[index]).astype(jnp.float32)
        for row in (index, levels + index):
            sums[row : row + 1, ch : ch + 128] = jnp.full((1, 128), cells, jnp.float32)

    pl.semaphore_wait(barrier, group - 1 + wide - 1)

    def exchange(tag, during):
        sent, first, held, second = ref["sums" + tag], ref["near" + tag], ref["held" + tag], ref["far" + tag]
        copies = []
        for step in range(1, group):
            copies.append(
                pltpu.make_async_remote_copy(
                    src_ref=sent,
                    dst_ref=first.at[g_me],
                    send_sem=ref["near_send" + tag].at[step - 1],
                    recv_sem=ref["near_recv" + tag].at[step - 1],
                    device_id=at_group(lax.rem(g_me + step, group)),
                    device_id_type=MESH,
                )
            )
            copies[-1].start()
        during[0]()
        own = sent[...]
        for copy in copies:
            copy.wait()
        total = None
        for source in range(group):
            term = jnp.where(source == g_me, own, first[source])
            total = term if total is None else total + term
        held[...] = total
        copies = []
        for step in range(1, wide):
            copies.append(
                pltpu.make_async_remote_copy(
                    src_ref=held,
                    dst_ref=second.at[w_me],
                    send_sem=ref["far_send" + tag].at[step - 1],
                    recv_sem=ref["far_recv" + tag].at[step - 1],
                    device_id=at_wide(lax.rem(w_me + step, wide)),
                    device_id_type=MESH,
                )
            )
            copies[-1].start()
        during[1]()
        own = held[...]
        for copy in copies:
            copy.wait()
        total = None
        for source in range(wide):
            term = jnp.where(source == w_me, own, second[source])
            total = term if total is None else total + term
        return total

    grads = ref["grads"]

    def take_grads():
        for index in range(levels):
            start, size = span(index)
            extent = extents[index]
            stage = ref[f"stage{index}"]
            loads[f"grad{index}"].wait()
            stage[:, 0:extent, :] = ref[f"grad{index}"][0].astype(jnp.float32)
            grads[start : start + size, :] = stage[...].reshape(size, ch) * masks[start : start + size, :]

    def turn():
        for number, segment in enumerate(segments):
            rows, pitch, base = segment["rows"], segment["pitch"], segment["base"]
            for row in range(0, rows, 128):
                block = xbs[number][pitch + row : pitch + row + 128, ch : 2 * ch]
                ref["turned"][:, base + row : base + row + 128] = block.astype(jnp.float32).T.astype(jnp.bfloat16)

    moments = exchange("1", (take_grads, turn))
    loads["gain"].wait()
    loads["shift"].wait()

    sums = ref["sums2"]
    scales, counts = [], []
    for index in range(levels):
        start, size = span(index)
        count = jnp.concatenate([moments[index : index + 1, ch : ch + 128]] * (ch // 128), axis=1)
        mean = moments[index : index + 1, 0:ch] / count
        variance = jnp.maximum(moments[levels + index : levels + index + 1, 0:ch] / count - mean * mean, 0.0)
        inverse = lax.rsqrt(variance + EPSILON)
        gain = ref["gain"][index : index + 1, :]
        shift = ref["shift"][index : index + 1, :]
        counts.append(count)
        scales.append(gain * inverse)
        shift_sum = jnp.zeros((8, ch), jnp.float32)
        gain_sum = jnp.zeros((8, ch), jnp.float32)
        for row in range(start, start + size, TILE):
            normed = (conv[row : row + TILE, :] - mean) * inverse
            shifted = gain * normed + shift
            sigma = 1.0 / (1.0 + jnp.exp(-shifted))
            slope = grads[row : row + TILE, :] * sigma * (1.0 + shifted * (1.0 - sigma))
            conv[row : row + TILE, :] = normed
            grads[row : row + TILE, :] = slope
            ref["acts"][row : row + TILE, :] = masks[row : row + TILE, :] * shifted * sigma
            shift_sum += fold(slope)
            gain_sum += fold(slope * normed)
        sums[index : index + 1, :] = jnp.sum(shift_sum, axis=0, keepdims=True)
        sums[levels + index : levels + index + 1, :] = jnp.sum(gain_sum, axis=0, keepdims=True)

    def put_acts():
        for index in range(levels):
            start, size = span(index)
            extent, pitch = extents[index], places[index][3]
            values = ref["acts"][start : start + size, :].reshape(extent, pitch, ch)
            ref[f"out{index}"][0] = values[:, 0:extent, :].astype(jnp.bfloat16)
            stores[f"out{index}"].start()

    slopes = exchange("2", (lambda: None, put_acts))
    ref["d_shift"][...] = slopes[0:levels, :] / devices
    ref["d_gain"][...] = slopes[levels : 2 * levels, :] / devices
    stores["d_shift"].start()
    stores["d_gain"].start()

    for index in range(levels):
        start, size = span(index)
        shift_term = slopes[index : index + 1, :] / counts[index]
        gain_term = slopes[levels + index : levels + index + 1, :] / counts[index]
        for row in range(start, start + size, TILE):
            grads[row : row + TILE, :] = (
                masks[row : row + TILE, :]
                * scales[index]
                * (grads[row : row + TILE, :] - shift_term - conv[row : row + TILE, :] * gain_term)
            )
        spread(bbs, index, grads[start : start + size, :])

    def weight_grad(tap):
        a, b = divmod(tap, 3)
        total = None
        for number, segment in enumerate(segments):
            rows, pitch, base = segment["rows"], segment["pitch"], segment["base"]
            part = jnp.dot(
                ref["turned"][:, base : base + rows],
                bbs[number][(2 - a) * pitch : (2 - a) * pitch + rows, (2 - b) * ch : (3 - b) * ch],
                preferred_element_type=jnp.float32,
            )
            total = part if total is None else total + part
        return total

    def input_grad(number, begin, count):
        pitch, base = segments[number]["pitch"], segments[number]["base"]
        total = None
        for a in range(3):
            for b in range(3):
                first = (2 - a) * pitch + begin
                part = lax.dot_general(
                    bbs[number][first : first + count, (2 - b) * ch : (3 - b) * ch],
                    weight[a, b],
                    (((1,), (1,)), ((), ())),
                    preferred_element_type=jnp.float32,
                )
                total = part if total is None else total + part
        where = slice(base + begin, base + begin + count)
        ref["acts"][where, :] = total * masks[where, :]

    def put_input_grads():
        for index in range(levels):
            start, size = span(index)
            extent, pitch = extents[index], places[index][3]
            values = ref["acts"][start : start + size, :].reshape(extent, pitch, ch)
            ref[f"d_feat{index}"][0] = values[:, 0:extent, :].astype(jnp.bfloat16)
            stores[f"d_feat{index}"].start()

    jobs = []
    for number, segment in enumerate(segments):
        tall = 256 if segment["rows"] % 256 == 0 else segment["rows"]
        for begin in range(0, segment["rows"], tall):
            jobs.append(functools.partial(input_grad, number, begin, tall))
    jobs.append(put_input_grads)

    if not shape["fused"]:
        for tap in range(9):
            ref["d_weight"][tap] = weight_grad(tap)
        for job in jobs:
            job()
        stores["d_weight"].start()
        for copy in stores.values():
            copy.wait()
        return

    part_ref, whole = ref["parts"], ref["d_weight"]
    core, y_me = lax.rem(g_me, 2), g_me // 2
    z_me, x_me = w_me // x_size, lax.rem(w_me, x_size)
    hops = {
        "core": Hop(2, core, lambda k: at_group(y_me * 2 + k)),
        "y": Hop(y_size, y_me, lambda k: at_group(k * 2 + core)),
        "x": Hop(x_size, x_me, lambda k: at_wide(z_me * x_size + k)),
        "z": Hop(z_size, z_me, lambda k: at_wide(k * x_size + x_me)),
    }

    class Chunk:
        def __init__(self, tap):
            self.tap = tap
            order = ("core", "x", "y", "z") if tap % 2 == 0 else ("core", "y", "x", "z")
            self.hops = [hops[name] for name in order]
            self.offsets, self.sizes = [0], [ch]
            for hop in self.hops:
                self.sizes.append(self.sizes[-1] // hop.size)
                self.offsets.append(self.offsets[-1] + hop.place * self.sizes[-1])
            self.flying = None

        def rows(self, offset, count):
            return pl.ds(pl.multiple_of(offset, 8), count)

        def sems(self, kind, level, step):
            before = sum(hop.size - 1 for hop in self.hops[:level]) + step - 1
            return ref[kind + "_send"].at[self.tap, before], ref[kind + "_recv"].at[self.tap, before]

        def scatter(self, level):
            hop, size = self.hops[level], self.sizes[level + 1]
            self.flying = []
            for step in range(1, hop.size):
                peer = lax.rem(hop.place + step, hop.size)
                send, recv = self.sems("rs", level, step)
                copy = pltpu.make_async_remote_copy(
                    src_ref=part_ref.at[self.tap, self.rows(self.offsets[level] + peer * size, size), :],
                    dst_ref=ref[f"land{level}"].at[self.tap, pl.ds((step - 1) * size, size), :],
                    send_sem=send,
                    recv_sem=recv,
                    device_id=hop.target(peer),
                    device_id_type=MESH,
                )
                copy.start()
                self.flying.append(copy)

        def gather(self, level):
            hop, size = self.hops[level], self.sizes[level + 1]
            mine = whole.at[self.tap, self.rows(self.offsets[level + 1], size), :]
            self.flying = []
            for step in range(1, hop.size):
                peer = lax.rem(hop.place + step, hop.size)
                send, recv = self.sems("ag", level, step)
                copy = pltpu.make_async_remote_copy(
                    src_ref=mine, dst_ref=mine, send_sem=send, recv_sem=recv,
                    device_id=hop.target(peer), device_id_type=MESH,
                )
                copy.start()
                self.flying.append(copy)

        def step(self, number):
            count = len(self.hops)
            if number == 0:
                part_ref[self.tap] = weight_grad(self.tap)
                self.scatter(0)
            elif number <= count:
                for copy in self.flying:
                    copy.wait()
                size = self.sizes[number]
                where = self.rows(self.offsets[number], size)
                total = part_ref[self.tap, where, :]
                for slot in range(self.hops[number - 1].size - 1):
                    total = total + ref[f"land{number - 1}"][self.tap, slot * size : (slot + 1) * size, :]
                if number < count:
                    part_ref[self.tap, where, :] = total
                    self.scatter(number)
                else:
                    whole[self.tap, where, :] = total / devices
                    self.gather(count - 1)
            else:
                for copy in self.flying:
                    copy.wait()
                if number < 2 * count:
                    self.gather(2 * count - 1 - number)

    chunks = [Chunk(tap) for tap in range(9)]
    for tap in range(9 + 2):
        if tap < 9:
            chunks[tap].step(0)
        if tap >= 2:
            chunks[tap - 2].step(1)
    turns = [(tap + SKEW * number, -number, tap) for tap in range(9) for number in range(2, 9)]
    for place, (_, number, tap) in enumerate(sorted(turns)):
        if jobs and place % 2 == 0:
            jobs.pop(0)()
        chunks[tap].step(-number)
    stores["d_weight"].start()
    for copy in stores.values():
        copy.wait()


def hand_on(arrays):
    count = len(arrays)

    def body(*refs):
        sources, targets, held = refs[:count], refs[count : 2 * count], refs[2 * count : 3 * count]
        read, write = refs[3 * count :]
        reads = [pltpu.make_async_copy(sources[i], held[i], read.at[i]) for i in range(count)]
        writes = [pltpu.make_async_copy(held[i], targets[i], write.at[i]) for i in range(count)]
        for copy in reads:
            copy.start()
        for first, second in zip(reads, writes):
            first.wait()
            second.start()
        for copy in writes:
            copy.wait()

    return list(
        pl.pallas_call(
            body,
            out_shape=[jax.ShapeDtypeStruct(array.shape, array.dtype) for array in arrays],
            in_specs=[pl.BlockSpec(memory_space=pl.ANY)] * count,
            out_specs=[pl.BlockSpec(memory_space=pl.ANY)] * count,
            scratch_shapes=[pltpu.VMEM(array.shape, array.dtype) for array in arrays]
            + [pltpu.SemaphoreType.DMA((count,))] * 2,
            compiler_params=pltpu.CompilerParams(vmem_limit_bytes=58 * 1024 * 1024),
        )(*arrays)
    )


def shards(mesh_shape, *arrays):
    feats, cots = arrays[0:4], arrays[4:8]
    weight, gain, shift, heights, widths = arrays[8:13]
    wide, group = mesh_shape["wide"], mesh_shape["group"]
    extents = tuple(feat.shape[1] for feat in feats)
    ch = weight.shape[3]
    devices = wide * group
    y_size = max(group // 2, 1)
    x_size = math.gcd(y_size, wide)
    z_size = wide // x_size
    fused = group == 2 * y_size and ch % (8 * devices) == 0
    segments, places, total_rows = plan(extents)
    levels = len(extents)
    smem = pl.BlockSpec(memory_space=pltpu.SMEM)

    names, ins = [], []

    def give(name, array, spec):
        names.append(name)
        ins.append((array, spec))

    hbm = pl.BlockSpec(memory_space=pltpu.HBM)
    for index in range(levels):
        give(f"feat{index}", feats[index], hbm)
    give("weight", weight, hbm)
    for index in range(levels):
        give(f"grad{index}", cots[index], hbm)
    give("gain", gain, hbm)
    give("shift", shift, hbm)
    loaded = tuple(names)
    give("heights", heights, smem)
    give("widths", widths, smem)

    outs = []
    for index in range(levels):
        names.append(f"out{index}")
        outs.append(jax.ShapeDtypeStruct(feats[index].shape, jnp.bfloat16))
    for index in range(levels):
        names.append(f"d_feat{index}")
        outs.append(jax.ShapeDtypeStruct(feats[index].shape, jnp.bfloat16))
    names.append("d_weight")
    outs.append(jax.ShapeDtypeStruct((9, ch, ch), jnp.float32))
    for name in ("d_gain", "d_shift"):
        names.append(name)
        outs.append(jax.ShapeDtypeStruct((levels, ch), jnp.float32))

    scratch = []
    stored = tuple(names[len(ins) :])

    def hold(name, kind):
        names.append(name)
        scratch.append(kind)

    f32 = jnp.float32
    for name, (array, _) in zip(loaded, ins):
        hold("vmem_" + name, pltpu.VMEM(array.shape, array.dtype))
    for name, out in zip(stored, outs):
        hold("vmem_" + name, pltpu.VMEM(out.shape, out.dtype))
    hold("store", pltpu.SemaphoreType.DMA((len(stored),)))
    hold("load", pltpu.SemaphoreType.DMA((len(loaded),)))
    for number, segment in enumerate(segments):
        tall = segment["rows"] + 2 * segment["pitch"]
        hold(f"xb{number}", pltpu.VMEM((tall, 3 * ch), jnp.bfloat16))
        hold(f"bb{number}", pltpu.VMEM((tall, 3 * ch), jnp.bfloat16))
    for index in range(levels):
        hold(f"stage{index}", pltpu.VMEM((extents[index], places[index][3], ch), f32))
    for name in ("masks", "conv", "grads", "acts"):
        hold(name, pltpu.VMEM((total_rows, ch), f32))
    hold("turned", pltpu.VMEM((ch, total_rows), jnp.bfloat16))
    for tag, across in (("1", ch + 128), ("2", ch)):
        hold("sums" + tag, pltpu.VMEM((2 * levels, across), f32))
        hold("held" + tag, pltpu.VMEM((2 * levels, across), f32))
        hold("near" + tag, pltpu.VMEM((group, 2 * levels, across), f32))
        hold("far" + tag, pltpu.VMEM((wide, 2 * levels, across), f32))
        for name, size in (("near", group), ("far", wide)):
            hold(f"{name}_send{tag}", pltpu.SemaphoreType.DMA((max(size - 1, 1),)))
            hold(f"{name}_recv{tag}", pltpu.SemaphoreType.DMA((max(size - 1, 1),)))
    if fused:
        hold("parts", pltpu.VMEM((9, ch, ch), f32))
        hold("land0", pltpu.VMEM((9, ch // 2, ch), f32))
        across = x_size
        rows = ch // 2
        hold("land1", pltpu.VMEM((9, rows // x_size * (x_size - 1), ch), f32))
        rows //= x_size
        hold("land2", pltpu.VMEM((9, rows // y_size * (y_size - 1), ch), f32))
        rows //= y_size
        hold("land3", pltpu.VMEM((9, rows // z_size * (z_size - 1), ch), f32))
        flights = 1 + x_size - 1 + y_size - 1 + z_size - 1
        for name in ("rs_send", "rs_recv", "ag_send", "ag_recv"):
            hold(name, pltpu.SemaphoreType.DMA((9, flights)))

    shape = dict(
        names=names, extents=extents, wide=wide, group=group, ch=ch,
        x=x_size, y=y_size, z=z_size, fused=fused, loaded=loaded, stored=stored,
    )
    results = pl.pallas_call(
        functools.partial(kernel, shape),
        out_shape=outs,
        in_specs=[spec for _, spec in ins],
        out_specs=[hbm] * len(outs),
        scratch_shapes=scratch,
        compiler_params=pltpu.CompilerParams(
            collective_id=0, has_side_effects=True, vmem_limit_bytes=58 * 1024 * 1024
        ),
    )(*[array for array, _ in ins])
    results = list(results)
    d_weight = results.pop(2 * levels)
    if fused:
        *results, d_weight = hand_on(results + [d_weight])
    else:
        results = hand_on(results)
        d_weight = lax.psum(d_weight, ("wide", "group")) / devices
    results.insert(2 * levels, d_weight.reshape(weight.shape))
    return tuple(results)


def solution(mesh):
    image = P(("wide", "group"), None, None, None)
    return jax.shard_map(
        functools.partial(shards, dict(mesh.shape)),
        mesh=mesh,
        in_specs=(image,) * 8 + (P(),) * 3 + (P(("wide", "group")),) * 2,
        out_specs=(image,) * 8 + (P(),) * 3,
        check_vma=False,
    )
```
